8 devices in a mesh: dp: 1 (over z), z: 2 (over y), y: 2 (over x), x: 2 (over core).
Axes of the slice: x: 2, y: 2, z: 1, core: 2. Of those that a mesh axis runs over, the one named last changes fastest.
Arguments:
- volume: bfloat16 [64, 48, 48, 48], P('dp', 'x', 'y', 'z')
- kernels: bfloat16 [3, 64, 64, 3, 3, 3], replicated
- biases: float32 [3, 64], replicated
Outputs:
- output: bfloat16 [64, 48, 48, 48], P('dp', 'x', 'y', 'z')
All inputs are finite; a program needn't handle non-finite values.
Results may differ from the reference program's by a relative error of at most 0.001.
Values are sent between devices in bfloat16 or wider.
A program may use at most 1 GiB of HBM per device.

```python
import jax
import jax.numpy as jnp
from jax import lax

CHANNELS = 64
KERNEL = 3
LAYERS = 3
GRID_X = 48
GRID_Y = 48
GRID_Z = 48
HALO_WIDTH = KERNEL // 2


def setup_inputs(seed: int = 0, part: int = 0) -> dict:
    root_key = jax.random.key(seed)
    vol_key, kernel_key, bias_key = jax.random.split(root_key, 3)
    fan_in = CHANNELS * KERNEL ** 3
    volume = jax.random.normal(jax.random.fold_in(vol_key, part), (CHANNELS, GRID_X, GRID_Y, GRID_Z), jnp.float32)
    kernels = jax.random.normal(kernel_key, (LAYERS, CHANNELS, CHANNELS, KERNEL, KERNEL, KERNEL), jnp.float32) * fan_in ** -0.5
    biases = 0.5 * jax.random.normal(bias_key, (LAYERS, CHANNELS), jnp.float32)
    return {"volume": volume.astype(jnp.bfloat16), "kernels": kernels.astype(jnp.bfloat16), "biases": biases}


def reference(volume, kernels, biases):
    pad_pairs = [(HALO_WIDTH, HALO_WIDTH)] * 3

    def apply_layer(current, layer_params):
        layer_kernel, layer_bias = layer_params
        conv_out = lax.conv_general_dilated(current.astype(jnp.float32)[None], layer_kernel.astype(jnp.float32), (1, 1, 1), pad_pairs, dimension_numbers=("NCDHW", "OIDHW", "NCDHW"), precision=lax.Precision.HIGHEST)[0]
        activated = jax.nn.gelu(conv_out + layer_bias[:, None, None, None])
        return (current.astype(jnp.float32) + activated).astype(jnp.bfloat16), None

    return lax.scan(apply_layer, volume, (kernels, biases))[0]
```

```python
import jax
import jax.numpy as jnp
from jax import lax
from jax.experimental import pallas as pl
from jax.experimental.pallas import tpu as pltpu
from jax.sharding import PartitionSpec as P

LAYERS, CH, TAPS, N = 3, 64, 9, 24
PAIRS = N // 2
SLABS = PAIRS + 1
PITCH, Z0 = 40, 8
GROUPS = ((1, 2), (3, 4), (5, 6), (7, 8), (9, 10), (11, 12))
SEND_LAG = 4
CHUNK = 2
WAIT_AHEAD = 1
F32, BF16 = jnp.float32, jnp.bfloat16


def kernel(vol, g_hbm, bias, out, v0, v1, v2, b_ref, io, g_v, wt, zsend, zrecv, crn,
           in_sem, g_sem, out_sem, send_sem, recv_sem):
    v = (v0, v1, v2)
    ix, iy, iz = lax.axis_index("x"), lax.axis_index("y"), lax.axis_index("z")

    def peer(*axes):
        mine = {"x": ix, "y": iy, "z": iz}
        return {a: 1 - mine[a] for a in axes}

    barrier = pltpu.get_barrier_semaphore()
    all_peers = (("x",), ("y",), ("z",), ("x", "y"), ("x", "z"), ("y", "z"), ("x", "y", "z"))
    for axes in all_peers:
        pl.semaphore_signal(barrier, inc=1, device_id=peer(*axes), device_id_type=pl.DeviceIdType.MESH)

    def plane0(j0, j1):
        return 2 * (ix * (j0 - 1) + (1 - ix) * (PAIRS - j1))

    def in_copy(i):
        j0, j1 = GROUPS[i]
        planes = pl.ds(plane0(j0, j1), 2 * (j1 - j0 + 1))
        return pltpu.make_async_copy(vol.at[planes], io.at[planes], in_sem.at[i])

    def out_copy(i):
        j0, j1 = GROUPS[i]
        planes = pl.ds(plane0(j0, j1), 2 * (j1 - j0 + 1))
        return pltpu.make_async_copy(io.at[planes], out.at[planes], out_sem.at[i])

    def g_copy(l):
        return pltpu.make_async_copy(g_hbm.at[l], g_v.at[l], g_sem.at[l])

    for i in range(len(GROUPS)):
        in_copy(i).start()
    for l in range(LAYERS):
        g_copy(l).start()

    def clear(j, carry):
        for l in range(LAYERS):
            v[l][j, 25 * iy, Z0:Z0 + N, :] = jnp.zeros((N, 128), F32)
        return carry

    lax.fori_loop(0, SLABS, clear, 0)

    y_src, y_dst = 1 + 23 * (1 - iy), 25 * iy
    kinds = 3 * len(GROUPS) + 4

    def remote(l, slot, src, dst, *axes):
        return pltpu.make_async_remote_copy(
            src_ref=src, dst_ref=dst, send_sem=send_sem.at[l * kinds + slot], recv_sem=recv_sem.at[l * kinds + slot],
            device_id=peer(*axes), device_id_type=pl.DeviceIdType.MESH)

    def copies(l, i):
        j0, j1 = GROUPS[i]
        slabs, rows, tile = pl.ds(j0, j1 - j0 + 1), pl.ds(Z0, N), pl.ds(16 * (1 - iy), 8)
        got = [
            remote(l, 3 * i, v[l].at[slabs, y_src, rows], v[l].at[slabs, y_dst, rows], "y"),
            remote(l, 3 * i + 1, zsend.at[l, slabs], zrecv.at[l, slabs], "z"),
            remote(l, 3 * i + 2, zsend.at[l, slabs, tile], crn.at[l, slabs], "y", "z"),
        ]
        if i == 0:
            n = 3 * len(GROUPS)
            got += [
                remote(l, n, v[l].at[1, pl.ds(1, N), rows], v[l].at[0, pl.ds(1, N), rows], "x"),
                remote(l, n + 1, v[l].at[1, y_src, rows], v[l].at[0, y_dst, rows], "x", "y"),
                remote(l, n + 2, zsend.at[l, 1], zrecv.at[l, 0], "x", "z"),
                remote(l, n + 3, zsend.at[l, 1, tile], crn.at[l, 0], "x", "y", "z"),
            ]
        return got

    def stage(l, j):
        lo, hi = v[l][j, 1:N + 1, Z0, :], v[l][j, 1:N + 1, Z0 + N - 1, :]
        zsend[l, j] = jnp.where(iz == 0, hi, lo)

    def send(l, i):
        j0, j1 = GROUPS[i]
        for j in range(j0, j1 + 1):
            stage(l, j)
        for c in copies(l, i):
            c.start()

    def fix(l, j):
        r, zero = zrecv[l, j], jnp.zeros((N, 128), F32)
        v[l][j, 1:N + 1, Z0 - 1, :] = jnp.where(iz == 1, r, zero)
        v[l][j, 1:N + 1, Z0 + N, :] = jnp.where(iz == 0, r, zero)
        for block, row, side in ((0, 7, 1), (25, 0, 0)):
            r = jnp.where(iy == side, crn[l, j, row:row + 1, :], zero[:1])
            v[l][j, block, Z0 - 1:Z0, :] = jnp.where(iz == 1, r, zero[:1])
            v[l][j, block, Z0 + N:Z0 + N + 1, :] = jnp.where(iz == 0, r, zero[:1])

    def receive(l, i):
        for c in copies(l, i):
            c.wait_recv()
        if i == 0:
            fix(l, 0)
        j0, j1 = GROUPS[i]
        for j in range(j0, j1 + 1):
            fix(l, j)

    def load_slab(j, carry):
        x = plane0(j, j)
        for y in range(0, N, 4):
            a, b = io[x, y:y + 4].astype(F32), io[x + 1, y:y + 4].astype(F32)
            v0[j, y + 1:y + 5, Z0:Z0 + N, :] = jnp.concatenate([a, b], axis=2)
        return carry

    def weights(l, carry):
        g_copy(l).wait()
        zero = jnp.zeros((CH, CH), F32)
        for t in range(TAPS):
            e, s = t // 3, t % 3
            ga, gb, gc = (g_v[l, a, e, s].astype(F32) for a in range(3))
            rows = (jnp.concatenate([gb, gc], axis=1), jnp.concatenate([ga, gb], axis=1),
                    jnp.concatenate([zero, ga], axis=1), jnp.concatenate([gc, zero], axis=1))
            for slot in range(4):
                wt[l, CH * slot:CH * slot + CH, 128 * t:128 * t + 128] = rows[slot]
        return carry

    prev = (lax.broadcasted_iota(jnp.int32, (CHUNK, N, 128), 2) < CH).astype(jnp.int32) == ix

    def finish(l, j):
        row = bias[l:l + 1, :]
        row = jnp.concatenate([row, row], axis=1).reshape(1, 1, 128)
        x = plane0(j, j)
        for y in range(0, N, CHUNK):
            ys = slice(y, y + CHUNK)
            blocks = slice(y + 1, y + 1 + CHUNK)
            after = b_ref[j + 1, ys, :, 128:] if j < PAIRS else jnp.zeros((CHUNK, N, 128), F32)
            acc = b_ref[j, ys, :, :128] + jnp.where(prev, b_ref[j - 1, ys, :, 128:], after) + row
            half = 0.5 * acc
            act = half + half * jnp.tanh(acc * (0.7978845608028654 + 0.035677408136300125 * (acc * acc)))
            new = v[l][j, blocks, Z0:Z0 + N, :] + act
            if l + 1 < LAYERS:
                v[l + 1][j, blocks, Z0:Z0 + N, :] = new.astype(BF16).astype(F32)
            else:
                io[x, ys] = new[:, :, :CH].astype(BF16)
                io[x + 1, ys] = pltpu.roll(new, CH, 2)[:, :, :CH].astype(BF16)

    def multiply(n):
        l, j = divmod(n, SLABS)
        parts = [v[l][j, t // 3:t // 3 + N, Z0 - 1 + t % 3:Z0 - 1 + t % 3 + N, :].reshape(N * N, 128) for t in range(TAPS)]
        prod = lax.dot_general(jnp.concatenate(parts, axis=1), wt[l], (((1,), (1,)), ((), ())), preferred_element_type=F32)
        b_ref[j] = prod.reshape(N, N, 256)

    pl.semaphore_wait(barrier, len(all_peers))
    for i, (j0, j1) in enumerate(GROUPS):
        in_copy(i).wait()
        lax.fori_loop(j0, j1 + 1, load_slab, 0)
        send(0, i)
    lax.fori_loop(0, LAYERS, weights, 0)

    last = LAYERS * SLABS
    for n in range(last + 4):
        for i, (j0, j1) in enumerate(GROUPS):
            for l in range(LAYERS):
                if n == max(0, l * SLABS + (j0 if i else 0) - WAIT_AHEAD):
                    receive(l, i)
                if n == l * SLABS + j1 + SEND_LAG and l + 1 < LAYERS:
                    send(l + 1, i)
            if n == (LAYERS - 1) * SLABS + j1 + 3:
                out_copy(i).start()
        if n < last:
            multiply(n)
        if 2 <= n <= last + 1 and (n - 2) % SLABS:
            finish(*divmod(n - 2, SLABS))
    for l in range(LAYERS):
        for i in range(len(GROUPS)):
            for c in copies(l, i):
                c.wait_send()
    for i in range(len(GROUPS)):
        out_copy(i).wait()


def solution(mesh):
    any_spec, vmem = pl.BlockSpec(memory_space=pl.ANY), pl.BlockSpec(memory_space=pltpu.VMEM)
    copies = LAYERS * (3 * len(GROUPS) + 4)

    def local(block, kernels, biases):
        vol = jnp.transpose(block, (1, 2, 3, 0))
        g = jnp.transpose(kernels, (0, 3, 4, 5, 1, 2))
        out = pl.pallas_call(
            kernel,
            out_shape=jax.ShapeDtypeStruct((N, N, N, CH), BF16),
            in_specs=[any_spec, any_spec, vmem],
            out_specs=any_spec,
            scratch_shapes=[pltpu.VMEM((SLABS, 26, PITCH, 128), F32)] * 3 + [
                pltpu.VMEM((SLABS, N, N, 256), F32),
                pltpu.VMEM((N, N, N, CH), BF16),
                pltpu.VMEM((LAYERS, 3, 3, 3, CH, CH), BF16),
                pltpu.VMEM((LAYERS, 256, 128 * TAPS), F32),
                pltpu.VMEM((LAYERS, SLABS, N, 128), F32),
                pltpu.VMEM((LAYERS, SLABS, N, 128), F32),
                pltpu.VMEM((LAYERS, SLABS, 8, 128), F32),
                pltpu.SemaphoreType.DMA((len(GROUPS),)),
                pltpu.SemaphoreType.DMA((LAYERS,)),
                pltpu.SemaphoreType.DMA((len(GROUPS),)),
                pltpu.SemaphoreType.DMA((copies,)),
                pltpu.SemaphoreType.DMA((copies,)),
            ],
            compiler_params=pltpu.CompilerParams(collective_id=0, has_side_effects=True, vmem_limit_bytes=60 * 2 ** 20),
        )(vol, g, biases)
        return jnp.transpose(out, (3, 0, 1, 2))

    spec = P("dp", "x", "y", "z")
    return jax.shard_map(local, mesh=mesh, in_specs=(spec, P(), P()), out_specs=spec, check_vma=False)
```

```python
import jax
import jax.numpy as jnp
from jax import lax
from jax.experimental import pallas as pl
from jax.experimental.pallas import tpu as pltpu
from jax.sharding import PartitionSpec as P

LAYERS, CH, TAPS, N = 3, 64, 9, 24
PAIRS = N // 2
SLABS = PAIRS + 1
PITCH, Z0 = 40, 8
ORDER = (1, 2, 3, 0, 4, 5, 6, 7, 8, 9, 10, 11, 12)
LOADS = ((1, 1), (2, 3), (4, 6), (7, 9), (10, 12))
FENCES = (1, 3, 5, 7, 9, 11)
CHUNK = 2
F32, BF16 = jnp.float32, jnp.bfloat16

PLACE = {j: p for p, j in enumerate(ORDER)}
READY = {j: max(PLACE[k] for k in (j - 1, j, j + 1) if k in PLACE) + 1 for j in range(1, SLABS)}
POINTS = [SLABS * l + p for l in range(-1, 2) for p in FENCES]


def _groups():
    found = {}
    for j in range(1, SLABS):
        key = (min(p for p in POINTS if p > READY[j]), max(p for p in POINTS if p <= SLABS + PLACE[j]))
        found.setdefault(key, []).append(j)
    return [(min(js), max(js), start, end) for (start, end), js in sorted(found.items(), key=lambda kv: kv[1])]


GROUPS = _groups()
X_END = max(p for p in POINTS if p <= SLABS + PLACE[0])


def kernel(vol, g_hbm, bias_hbm, out, v0, v1, v2, b_ref, io, g_v, wt, zsend, zrecv, ysend, yrecv, xsend, xrecv,
           csend, crecv, bias, in_sem, bias_sem, g_sem, send_sem, recv_sem):
    v = (v0, v1, v2)
    ip, ib, iz = lax.axis_index("y"), lax.axis_index("x"), lax.axis_index("z")

    def peer(*axes):
        mine = {"y": ip, "x": ib, "z": iz}
        return {a: 1 - mine[a] for a in axes}

    barrier = pltpu.get_barrier_semaphore()
    all_peers = (("x",), ("y",), ("z",), ("x", "y"), ("x", "z"), ("y", "z"), ("x", "y", "z"))
    for axes in all_peers:
        pl.semaphore_signal(barrier, inc=1, device_id=peer(*axes), device_id_type=pl.DeviceIdType.MESH)

    def plane0(j0, j1):
        return 2 * (ip * (j0 - 1) + (1 - ip) * (PAIRS - j1))

    def in_copy(i):
        j0, j1 = LOADS[i]
        planes = pl.ds(plane0(j0, j1), 2 * (j1 - j0 + 1))
        return pltpu.make_async_copy(vol.at[:, planes], io.at[:, planes], in_sem.at[i])

    def g_copy(l):
        return pltpu.make_async_copy(g_hbm.at[l], g_v.at[l], g_sem.at[l])

    for i in range(len(LOADS)):
        in_copy(i).start()
    for l in range(LAYERS):
        g_copy(l).start()
    bias_copy = pltpu.make_async_copy(bias_hbm, bias, bias_sem)
    bias_copy.start()

    y_src = 1 + (N - 1) * (1 - ib)
    kinds = 3 * len(GROUPS) + 4

    def remote(l, slot, src, dst, *axes):
        return pltpu.make_async_remote_copy(
            src_ref=src, dst_ref=dst, send_sem=send_sem.at[l * kinds + slot], recv_sem=recv_sem.at[l * kinds + slot],
            device_id=peer(*axes), device_id_type=pl.DeviceIdType.MESH)

    def copies(l, i):
        j0, j1 = GROUPS[i][:2]
        slabs = pl.ds(j0, j1 - j0 + 1)
        got = [
            remote(l, 3 * i, ysend.at[l, slabs], yrecv.at[l, slabs], "x"),
            remote(l, 3 * i + 1, zsend.at[l, slabs], zrecv.at[l, slabs], "z"),
            remote(l, 3 * i + 2, csend.at[l, slabs], crecv.at[l, slabs], "x", "z"),
        ]
        if i == 0:
            n = 3 * len(GROUPS)
            got += [
                remote(l, n, xsend.at[l], xrecv.at[l], "y"),
                remote(l, n + 1, ysend.at[l, 1], yrecv.at[l, 0], "x", "y"),
                remote(l, n + 2, zsend.at[l, 1], zrecv.at[l, 0], "y", "z"),
                remote(l, n + 3, csend.at[l, 1], crecv.at[l, 0], "x", "y", "z"),
            ]
        return got

    near = (lax.broadcasted_iota(jnp.int32, (N // 2, N, 128), 2) < CH).astype(jnp.int32) == ip

    def stage(l, j):
        lo, hi = v[l][j, 1:N + 1, Z0, :], v[l][j, 1:N + 1, Z0 + N - 1, :]
        edge = jnp.where(iz == 0, hi, lo)
        zsend[l, j] = edge.astype(BF16)
        ysend[l, j] = v[l][j, y_src, Z0:Z0 + N, :].astype(BF16)
        csend[l, j, 0:1] = jnp.where(ib == 0, edge[N - 1:N], edge[0:1])
        if j == 1:
            half = N // 2
            a, b = v[l][1, 1:half + 1, Z0:Z0 + N, :], v[l][1, half + 1:N + 1, Z0:Z0 + N, :]
            stay, move = jnp.where(ip == 1, a, b), jnp.where(ip == 1, b, a)
            xsend[l] = jnp.where(near, stay, pltpu.roll(move, CH, 2)).astype(BF16)

    def send(l, i):
        j0, j1 = GROUPS[i][:2]
        for j in range(j0, j1 + 1):
            stage(l, j)
        for c in copies(l, i):
            c.start()

    def fix(l, j):
        zero = jnp.zeros((N, 128), F32)
        r = zrecv[l, j].astype(F32)
        v[l][j, 1:N + 1, Z0 - 1, :] = jnp.where(iz == 1, r, zero)
        v[l][j, 1:N + 1, Z0 + N, :] = jnp.where(iz == 0, r, zero)
        r, c = yrecv[l, j].astype(F32), crecv[l, j, 0:1, :]
        for block, side in ((0, 1), (N + 1, 0)):
            v[l][j, block, Z0:Z0 + N, :] = jnp.where(ib == side, r, zero)
            corner = jnp.where(ib == side, c, zero[:1])
            v[l][j, block, Z0 - 1:Z0, :] = jnp.where(iz == 1, corner, zero[:1])
            v[l][j, block, Z0 + N:Z0 + N + 1, :] = jnp.where(iz == 0, corner, zero[:1])
        if j == 0:
            half = N // 2
            r = xrecv[l].astype(F32)
            t = pltpu.roll(r, CH, 2)
            v[l][0, 1:half + 1, Z0:Z0 + N, :] = jnp.where(ip == 0, r, t)
            v[l][0, half + 1:N + 1, Z0:Z0 + N, :] = jnp.where(ip == 0, t, r)

    def receive(l, i):
        for c in copies(l, i)[:3]:
            c.wait_recv()
        j0, j1 = GROUPS[i][:2]
        for j in range(j0, j1 + 1):
            fix(l, j)

    def receive_x(l):
        for c in copies(l, 0)[3:]:
            c.wait_recv()
        fix(l, 0)

    def load_slab(j, carry):
        x = plane0(j, j)
        for y in range(0, N, 4):
            a, b = io[y:y + 4, x].astype(F32), io[y:y + 4, x + 1].astype(F32)
            v0[j, y + 1:y + 5, Z0:Z0 + N, :] = jnp.concatenate([a, b], axis=2)
        return carry

    def weights(l, carry):
        g_copy(l).wait()
        zero = jnp.zeros((CH, CH), F32)
        for t in range(TAPS):
            e, s = t // 3, t % 3
            ga, gb, gc = (g_v[l, e, a, s].astype(F32) for a in range(3))
            rows = (jnp.concatenate([gb, gc], axis=1), jnp.concatenate([ga, gb], axis=1),
                    jnp.concatenate([zero, ga], axis=1), jnp.concatenate([gc, zero], axis=1))
            for slot in range(4):
                wt[l, CH * slot:CH * slot + CH, 128 * t:128 * t + 128] = rows[slot]
        return carry

    prev = (lax.broadcasted_iota(jnp.int32, (CHUNK, N, 128), 2) < CH).astype(jnp.int32) == ip

    def finish(l, j):
        row = bias[l:l + 1, :]
        row = jnp.concatenate([row, row], axis=1).reshape(1, 1, 128)
        x = plane0(j, j)
        for y in range(0, N, CHUNK):
            ys = slice(y, y + CHUNK)
            blocks = slice(y + 1, y + 1 + CHUNK)
            after = b_ref[j + 1, ys, :, 128:] if j < PAIRS else jnp.zeros((CHUNK, N, 128), F32)
            acc = b_ref[j, ys, :, :128] + jnp.where(prev, b_ref[j - 1, ys, :, 128:], after) + row
            half = 0.5 * acc
            act = half + half * jnp.tanh(acc * (0.7978845608028654 + 0.035677408136300125 * (acc * acc)))
            new = v[l][j, blocks, Z0:Z0 + N, :] + act
            if l + 1 < LAYERS:
                v[l + 1][j, blocks, Z0:Z0 + N, :] = new.astype(BF16).astype(F32)
            else:
                out[ys, x] = new[:, :, :CH].astype(BF16)
                out[ys, x + 1] = pltpu.roll(new, CH, 2)[:, :, :CH].astype(BF16)

    def multiply(l, j):
        parts = [v[l][j, t // 3:t // 3 + N, Z0 - 1 + t % 3:Z0 - 1 + t % 3 + N, :].reshape(N * N, 128) for t in range(TAPS)]
        prod = lax.dot_general(jnp.concatenate(parts, axis=1), wt[l], (((1,), (1,)), ((), ())), preferred_element_type=F32)
        b_ref[j] = prod.reshape(N, N, 256)

    pl.semaphore_wait(barrier, len(all_peers))
    done = 0
    for i, (j0, j1) in enumerate(LOADS):
        in_copy(i).wait()
        lax.fori_loop(j0, j1 + 1, load_slab, 0)
        while done < len(GROUPS) and GROUPS[done][1] <= j1:
            send(0, done)
            done += 1
    lax.fori_loop(0, LAYERS, weights, 0)
    bias_copy.wait()

    for n in range(LAYERS * SLABS + 2):
        for l in range(1, LAYERS):
            for i, (_, _, start, _) in enumerate(GROUPS):
                if n == (l - 1) * SLABS + start:
                    send(l, i)
        for l in range(LAYERS):
            for i, (_, _, _, end) in enumerate(GROUPS):
                if n == max(0, (l - 1) * SLABS + end):
                    receive(l, i)
            if n == max(0, (l - 1) * SLABS + X_END):
                receive_x(l)
        if n < LAYERS * SLABS:
            multiply(n // SLABS, ORDER[n % SLABS])
        for l in range(LAYERS):
            for j in range(1, SLABS):
                if n - l * SLABS == READY[j]:
                    finish(l, j)
    for l in range(LAYERS):
        for i in range(len(GROUPS)):
            for c in copies(l, i):
                c.wait_send()


def solution(mesh):
    any_spec, vmem = pl.BlockSpec(memory_space=pl.ANY), pl.BlockSpec(memory_space=pltpu.VMEM)
    copies = LAYERS * (3 * len(GROUPS) + 4)

    def local(block, kernels, biases):
        vol = jnp.transpose(block, (1, 2, 3, 0))
        g = jnp.transpose(kernels, (0, 3, 4, 5, 1, 2))
        out = pl.pallas_call(
            kernel,
            out_shape=pltpu.VMEM((N, N, N, CH), BF16),
            in_specs=[any_spec] * 3,
            out_specs=vmem,
            scratch_shapes=[pltpu.VMEM((SLABS, 26, PITCH, 128), F32)] * 3 + [
                pltpu.VMEM((SLABS, N, N, 256), F32),
                pltpu.VMEM((N, N, N, CH), BF16),
                pltpu.VMEM((LAYERS, 3, 3, 3, CH, CH), BF16),
                pltpu.VMEM((LAYERS, 256, 128 * TAPS), F32),
                pltpu.VMEM((LAYERS, SLABS, N, 128), BF16),
                pltpu.VMEM((LAYERS, SLABS, N, 128), BF16),
                pltpu.VMEM((LAYERS, SLABS, N, 128), BF16),
                pltpu.VMEM((LAYERS, SLABS, N, 128), BF16),
                pltpu.VMEM((LAYERS, N // 2, N, 128), BF16),
                pltpu.VMEM((LAYERS, N // 2, N, 128), BF16),
                pltpu.VMEM((LAYERS, SLABS, 8, 128), F32),
                pltpu.VMEM((LAYERS, SLABS, 8, 128), F32),
                pltpu.VMEM((LAYERS, CH), F32),
                pltpu.SemaphoreType.DMA((len(LOADS),)),
                pltpu.SemaphoreType.DMA,
                pltpu.SemaphoreType.DMA((LAYERS,)),
                pltpu.SemaphoreType.DMA((copies,)),
                pltpu.SemaphoreType.DMA((copies,)),
            ],
            compiler_params=pltpu.CompilerParams(collective_id=0, has_side_effects=True, vmem_limit_bytes=52 * 2 ** 20),
        )(vol, g, biases)
        return jnp.transpose(out, (3, 0, 1, 2))

    spec = P("dp", "x", "y", "z")
    return jax.shard_map(local, mesh=mesh, in_specs=(spec, P(), P()), out_specs=spec, check_vma=False)
```

```python
import jax
import jax.numpy as jnp
from jax import lax
from jax.experimental import pallas as pl
from jax.experimental.pallas import tpu as pltpu
from jax.sharding import PartitionSpec as P

LAYERS, CH, TAPS, N = 3, 64, 9, 24
PAIRS = N // 2
SLABS = PAIRS + 1
PITCH, Z0 = 40, 8
ORDER = (1, 2, 3, 0, 4, 5, 6, 7, 8, 9, 10, 11, 12)
LOADS = ((1, 1), (2, 3), (4, 6), (7, 9), (10, 12))
FENCES = (1, 3, 5, 7, 9, 11)
CHUNK = 2
AHEAD = 0
F32, BF16 = jnp.float32, jnp.bfloat16

PLACE = {j: p for p, j in enumerate(ORDER)}
READY = {j: max(PLACE[k] for k in (j - 1, j, j + 1) if k in PLACE) + 1 for j in range(1, SLABS)}
POINTS = [SLABS * l + p for l in range(-1, 2) for p in FENCES]


def _groups():
    found = {}
    for j in range(1, SLABS):
        key = (min(p for p in POINTS if p > READY[j]), max(p for p in POINTS if p <= SLABS + PLACE[j] - AHEAD))
        found.setdefault(key, []).append(j)
    return [(min(js), max(js), start, end) for (start, end), js in sorted(found.items(), key=lambda kv: kv[1])]


GROUPS = _groups()
X_END = max(p for p in POINTS if p <= SLABS + PLACE[0] - AHEAD)
PART = {j: (i, j - g[0]) for i, g in enumerate(GROUPS) for j in range(g[0], g[1] + 1)}


def kernel(vol, g_hbm, bias_hbm, out, v0, v1, v2, b_ref, io, g_v, wt, zsend, zrecv, ysend, yrecv, xsend, xrecv,
           csend, crecv, drecv, bias, in_sem, bias_sem, g_sem, send_sem, recv_sem):
    v = (v0, v1, v2)
    ip, ib, iz = lax.axis_index("y"), lax.axis_index("x"), lax.axis_index("z")

    def peer(*axes):
        mine = {"y": ip, "x": ib, "z": iz}
        return {a: 1 - mine[a] for a in axes}

    barrier = pltpu.get_barrier_semaphore()
    all_peers = (("x",), ("y",), ("z",), ("x", "y"), ("x", "z"), ("y", "z"), ("x", "y", "z"))
    for axes in all_peers:
        pl.semaphore_signal(barrier, inc=1, device_id=peer(*axes), device_id_type=pl.DeviceIdType.MESH)

    def plane0(j0, j1):
        return 2 * (ip * (j0 - 1) + (1 - ip) * (PAIRS - j1))

    def in_copy(i):
        j0, j1 = LOADS[i]
        planes = pl.ds(plane0(j0, j1), 2 * (j1 - j0 + 1))
        return pltpu.make_async_copy(vol.at[:, planes], io.at[:, planes], in_sem.at[i])

    def g_copy(l):
        return pltpu.make_async_copy(g_hbm.at[l], g_v.at[l], g_sem.at[l])

    for i in range(len(LOADS)):
        in_copy(i).start()
    for l in range(LAYERS):
        g_copy(l).start()
    bias_copy = pltpu.make_async_copy(bias_hbm, bias, bias_sem)
    bias_copy.start()

    kinds = 3 * len(GROUPS) + 4

    def remote(l, slot, src, dst, *axes):
        return pltpu.make_async_remote_copy(
            src_ref=src, dst_ref=dst, send_sem=send_sem.at[l * kinds + slot], recv_sem=recv_sem.at[l * kinds + slot],
            device_id=peer(*axes), device_id_type=pl.DeviceIdType.MESH)

    def copies(l, i):
        j0, j1 = GROUPS[i][:2]
        slabs = pl.ds(j0, j1 - j0 + 1)
        got = [
            remote(l, 3 * i, ysend.at[l, slabs], yrecv.at[l, slabs], "x"),
            remote(l, 3 * i + 1, zsend.at[l, slabs], zrecv.at[l, slabs], "z"),
            remote(l, 3 * i + 2, csend.at[l, i], crecv.at[l, i], "x", "z"),
        ]
        if i == 0:
            n = 3 * len(GROUPS)
            got += [
                remote(l, n, xsend.at[l], xrecv.at[l], "y"),
                remote(l, n + 1, ysend.at[l, 1], yrecv.at[l, 0], "x", "y"),
                remote(l, n + 2, zsend.at[l, 1], zrecv.at[l, 0], "y", "z"),
                remote(l, n + 3, csend.at[l, 0], drecv.at[l], "x", "y", "z"),
            ]
        return got

    near = (lax.broadcasted_iota(jnp.int32, (N // 2, N, 128), 2) < CH).astype(jnp.int32) == ip

    def stage(l, j):
        lo, hi = v[l][j, 1:N + 1, Z0, :], v[l][j, 1:N + 1, Z0 + N - 1, :]
        edge = jnp.where(iz == 0, hi, lo)
        zsend[l, j] = edge.astype(BF16)
        ysend[l, j] = jnp.where(ib == 0, v[l][j, N, Z0:Z0 + N, :], v[l][j, 1, Z0:Z0 + N, :]).astype(BF16)
        i, r = PART[j]
        csend[l, i, r:r + 1] = jnp.where(ib == 0, edge[N - 1:N], edge[0:1])
        if j == 1:
            half = N // 2
            a, b = v[l][1, 1:half + 1, Z0:Z0 + N, :], v[l][1, half + 1:N + 1, Z0:Z0 + N, :]
            stay, move = jnp.where(ip == 1, a, b), jnp.where(ip == 1, b, a)
            xsend[l] = jnp.where(near, stay, pltpu.roll(move, CH, 2)).astype(BF16)

    def send(l, i):
        for c in copies(l, i):
            c.start()

    def fix(l, j):
        zero = jnp.zeros((N, 128), F32)
        r = zrecv[l, j].astype(F32)
        v[l][j, 1:N + 1, Z0 - 1, :] = jnp.where(iz == 1, r, zero)
        v[l][j, 1:N + 1, Z0 + N, :] = jnp.where(iz == 0, r, zero)
        r = yrecv[l, j].astype(F32)
        i, k = PART[j] if j else (0, 0)
        c = crecv[l, i, k:k + 1, :] if j else drecv[l, 0:1, :]
        for block, side in ((0, 1), (N + 1, 0)):
            v[l][j, block, Z0:Z0 + N, :] = jnp.where(ib == side, r, zero)
            corner = jnp.where(ib == side, c, zero[:1])
            v[l][j, block, Z0 - 1:Z0, :] = jnp.where(iz == 1, corner, zero[:1])
            v[l][j, block, Z0 + N:Z0 + N + 1, :] = jnp.where(iz == 0, corner, zero[:1])
        if j == 0:
            half = N // 2
            r = xrecv[l].astype(F32)
            t = pltpu.roll(r, CH, 2)
            v[l][0, 1:half + 1, Z0:Z0 + N, :] = jnp.where(ip == 0, r, t)
            v[l][0, half + 1:N + 1, Z0:Z0 + N, :] = jnp.where(ip == 0, t, r)

    def receive(l, i):
        for c in copies(l, i)[:3]:
            c.wait_recv()

    def receive_x(l):
        for c in copies(l, 0)[3:]:
            c.wait_recv()

    def load_slab(j, carry):
        x = plane0(j, j)
        for y in range(0, N, 4):
            a, b = io[y:y + 4, x].astype(F32), io[y:y + 4, x + 1].astype(F32)
            v0[j, y + 1:y + 5, Z0:Z0 + N, :] = jnp.concatenate([a, b], axis=2)
        return carry

    def weights(l, carry):
        g_copy(l).wait()
        zero = jnp.zeros((CH, CH), F32)
        for t in range(TAPS):
            e, s = t // 3, t % 3
            ga, gb, gc = (g_v[l, e, a, s].astype(F32) for a in range(3))
            rows = (jnp.concatenate([gb, gc], axis=1), jnp.concatenate([ga, gb], axis=1),
                    jnp.concatenate([zero, ga], axis=1), jnp.concatenate([gc, zero], axis=1))
            for slot in range(4):
                wt[l, CH * slot:CH * slot + CH, 128 * t:128 * t + 128] = rows[slot]
        return carry

    prev = (lax.broadcasted_iota(jnp.int32, (CHUNK, N, 128), 2) < CH).astype(jnp.int32) == ip

    def finish(l, j):
        row = bias[l:l + 1, :]
        row = jnp.concatenate([row, row], axis=1).reshape(1, 1, 128)
        x = plane0(j, j)
        for y in range(0, N, CHUNK):
            ys = slice(y, y + CHUNK)
            blocks = slice(y + 1, y + 1 + CHUNK)
            after = b_ref[j + 1, ys, :, 128:] if j < PAIRS else jnp.zeros((CHUNK, N, 128), F32)
            acc = b_ref[j, ys, :, :128] + jnp.where(prev, b_ref[j - 1, ys, :, 128:], after) + row
            half = 0.5 * acc
            act = half + half * jnp.tanh(acc * (0.7978845608028654 + 0.035677408136300125 * (acc * acc)))
            new = v[l][j, blocks, Z0:Z0 + N, :] + act
            if l + 1 < LAYERS:
                v[l + 1][j, blocks, Z0:Z0 + N, :] = new.astype(BF16).astype(F32)
            else:
                out[ys, x] = new[:, :, :CH].astype(BF16)
                out[ys, x + 1] = pltpu.roll(new, CH, 2)[:, :, :CH].astype(BF16)

    def multiply(l, j):
        parts = [v[l][j, t // 3:t // 3 + N, Z0 - 1 + t % 3:Z0 - 1 + t % 3 + N, :].reshape(N * N, 128) for t in range(TAPS)]
        prod = lax.dot_general(jnp.concatenate(parts, axis=1), wt[l], (((1,), (1,)), ((), ())), preferred_element_type=F32)
        b_ref[j] = prod.reshape(N, N, 256)

    done = 0
    for i, (j0, j1) in enumerate(LOADS):
        in_copy(i).wait()
        lax.fori_loop(j0, j1 + 1, load_slab, 0)
        while done < len(GROUPS) and GROUPS[done][1] <= j1:
            for j in range(GROUPS[done][0], GROUPS[done][1] + 1):
                stage(0, j)
            if done == 0:
                pl.semaphore_wait(barrier, len(all_peers))
            send(0, done)
            done += 1
    lax.fori_loop(0, LAYERS, weights, 0)
    bias_copy.wait()

    for n in range(LAYERS * SLABS + 2):
        for l in range(1, LAYERS):
            for i, (_, _, start, _) in enumerate(GROUPS):
                if n == (l - 1) * SLABS + start:
                    send(l, i)
        arrived = []
        for l in range(LAYERS):
            for i, (j0, j1, _, end) in enumerate(GROUPS):
                if n == max(0, (l - 1) * SLABS + end):
                    receive(l, i)
                    arrived += [(l, j) for j in range(j0, j1 + 1)]
            if n == max(0, (l - 1) * SLABS + X_END):
                receive_x(l)
                arrived.append((l, 0))
        for l in range(LAYERS):
            for j in range(1, SLABS):
                if n - l * SLABS == READY[j]:
                    finish(l, j)
                    if l + 1 < LAYERS:
                        stage(l + 1, j)
        for l, j in arrived:
            fix(l, j)
        if n < LAYERS * SLABS:
            multiply(n // SLABS, ORDER[n % SLABS])
    for l in range(LAYERS):
        for i in range(len(GROUPS)):
            for c in copies(l, i):
                c.wait_send()


def solution(mesh):
    any_spec, vmem = pl.BlockSpec(memory_space=pl.ANY), pl.BlockSpec(memory_space=pltpu.VMEM)
    copies = LAYERS * (3 * len(GROUPS) + 4)

    def local(block, kernels, biases):
        vol = jnp.transpose(block, (1, 2, 3, 0))
        g = jnp.transpose(kernels, (0, 3, 4, 5, 1, 2))
        out = pl.pallas_call(
            kernel,
            out_shape=pltpu.VMEM((N, N, N, CH), BF16),
            in_specs=[any_spec] * 3,
            out_specs=vmem,
            scratch_shapes=[pltpu.VMEM((SLABS, 26, PITCH, 128), F32)] * 3 + [
                pltpu.VMEM((SLABS, N, N, 256), F32),
                pltpu.VMEM((N, N, N, CH), BF16),
                pltpu.VMEM((LAYERS, 3, 3, 3, CH, CH), BF16),
                pltpu.VMEM((LAYERS, 256, 128 * TAPS), F32),
                pltpu.VMEM((LAYERS, SLABS, N, 128), BF16),
                pltpu.VMEM((LAYERS, SLABS, N, 128), BF16),
                pltpu.VMEM((LAYERS, SLABS, N, 128), BF16),
                pltpu.VMEM((LAYERS, SLABS, N, 128), BF16),
                pltpu.VMEM((LAYERS, N // 2, N, 128), BF16),
                pltpu.VMEM((LAYERS, N // 2, N, 128), BF16),
                pltpu.VMEM((LAYERS, len(GROUPS), 8, 128), F32),
                pltpu.VMEM((LAYERS, len(GROUPS), 8, 128), F32),
                pltpu.VMEM((LAYERS, 8, 128), F32),
                pltpu.VMEM((LAYERS, CH), F32),
                pltpu.SemaphoreType.DMA((len(LOADS),)),
                pltpu.SemaphoreType.DMA,
                pltpu.SemaphoreType.DMA((LAYERS,)),
                pltpu.SemaphoreType.DMA((copies,)),
                pltpu.SemaphoreType.DMA((copies,)),
            ],
            compiler_params=pltpu.CompilerParams(collective_id=0, has_side_effects=True, vmem_limit_bytes=52 * 2 ** 20),
        )(vol, g, biases)
        return jnp.transpose(out, (3, 0, 1, 2))

    spec = P("dp", "x", "y", "z")
    return jax.shard_map(local, mesh=mesh, in_specs=(spec, P(), P()), out_specs=spec, check_vma=False)
```

```python
import jax
import jax.numpy as jnp
from jax import lax
from jax.experimental import pallas as pl
from jax.experimental.pallas import tpu as pltpu
from jax.sharding import PartitionSpec as P

LAYERS, CH, TAPS, N = 3, 64, 9, 24
PAIRS = N // 2
SLABS = PAIRS + 1
PITCH, Z0 = 40, 8
ORDER = (1, 2, 3, 0, 4, 5, 6, 7, 8, 9, 10, 11, 12)
LOADS = ((1, 1), (2, 3), (4, 6), (7, 9), (10, 12))
FENCES = (1, 3, 5, 7, 9, 11)
CHUNK = 2
AHEAD = 0
F32, BF16 = jnp.float32, jnp.bfloat16

PLACE = {j: p for p, j in enumerate(ORDER)}
READY = {j: max(PLACE[k] for k in (j - 1, j, j + 1) if k in PLACE) + 1 for j in range(1, SLABS)}
POINTS = [SLABS * l + p for l in range(-1, 2) for p in FENCES]


def _groups():
    found = {}
    for j in range(1, SLABS):
        key = (min(p for p in POINTS if p > READY[j]), max(p for p in POINTS if p <= SLABS + PLACE[j] - AHEAD))
        found.setdefault(key, []).append(j)
    return [(min(js), max(js), start, end) for (start, end), js in sorted(found.items(), key=lambda kv: kv[1])]


GROUPS = _groups()
X_END = max(p for p in POINTS if p <= SLABS + PLACE[0] - AHEAD)
PART = {j: (i, j - g[0]) for i, g in enumerate(GROUPS) for j in range(g[0], g[1] + 1)}


def kernel(vol, g_hbm, bias_hbm, out, v0, v1, v2, b_ref, io, g_v, wt, zsend, zrecv, ysend, yrecv, xsend, xrecv,
           csend, crecv, drecv, bias, in_sem, bias_sem, g_sem, send_sem, recv_sem):
    v = (v0, v1, v2)
    ip, ib, iz = lax.axis_index("y"), lax.axis_index("x"), lax.axis_index("z")

    def peer(*axes):
        mine = {"y": ip, "x": ib, "z": iz}
        return {a: 1 - mine[a] for a in axes}

    barrier = pltpu.get_barrier_semaphore()
    all_peers = (("x",), ("y",), ("z",), ("x", "y"), ("x", "z"), ("y", "z"), ("x", "y", "z"))
    for axes in all_peers:
        pl.semaphore_signal(barrier, inc=1, device_id=peer(*axes), device_id_type=pl.DeviceIdType.MESH)

    def plane0(j0, j1):
        return 2 * (ip * (j0 - 1) + (1 - ip) * (PAIRS - j1))

    def in_copy(i):
        j0, j1 = LOADS[i]
        planes = pl.ds(plane0(j0, j1), 2 * (j1 - j0 + 1))
        return pltpu.make_async_copy(vol.at[:, planes], io.at[:, planes], in_sem.at[i])

    def g_copy(l):
        return pltpu.make_async_copy(g_hbm.at[l], g_v.at[l], g_sem.at[l])

    for i in range(len(LOADS)):
        in_copy(i).start()
    for l in range(LAYERS):
        g_copy(l).start()
    bias_copy = pltpu.make_async_copy(bias_hbm, bias, bias_sem)
    bias_copy.start()

    kinds = 3 * len(GROUPS) + 4

    def remote(l, slot, src, dst, *axes):
        return pltpu.make_async_remote_copy(
            src_ref=src, dst_ref=dst, send_sem=send_sem.at[l * kinds + slot], recv_sem=recv_sem.at[l * kinds + slot],
            device_id=peer(*axes), device_id_type=pl.DeviceIdType.MESH)

    def copies(l, i):
        j0, j1 = GROUPS[i][:2]
        slabs = pl.ds(j0, j1 - j0 + 1)
        got = [
            remote(l, 3 * i, ysend.at[l, slabs], yrecv.at[l, slabs], "x"),
            remote(l, 3 * i + 1, zsend.at[l, slabs], zrecv.at[l, slabs], "z"),
            remote(l, 3 * i + 2, csend.at[l, i], crecv.at[l, i], "x", "z"),
        ]
        if i == 0:
            n = 3 * len(GROUPS)
            got += [
                remote(l, n, xsend.at[l], xrecv.at[l], "y"),
                remote(l, n + 1, ysend.at[l, 1], yrecv.at[l, 0], "x", "y"),
                remote(l, n + 2, zsend.at[l, 1], zrecv.at[l, 0], "y", "z"),
                remote(l, n + 3, csend.at[l, 0], drecv.at[l], "x", "y", "z"),
            ]
        return got

    near = (lax.broadcasted_iota(jnp.int32, (N // 2, N, 128), 2) < CH).astype(jnp.int32) == ip

    def flat(l):
        return v[l].reshape(SLABS * (N + 2) * PITCH, 128)

    def column(j, row):
        return pl.ds((j * (N + 2) + 1) * PITCH + row, N, stride=PITCH)

    def stage(l, j):
        lo, hi = flat(l)[column(j, Z0), :], flat(l)[column(j, Z0 + N - 1), :]
        edge = jnp.where(iz == 0, hi, lo)
        zsend[l, j] = edge.astype(BF16)
        ysend[l, j] = jnp.where(ib == 0, v[l][j, N, Z0:Z0 + N, :], v[l][j, 1, Z0:Z0 + N, :]).astype(BF16)
        i, r = PART[j]
        csend[l, i, r:r + 1] = jnp.where(ib == 0, edge[N - 1:N], edge[0:1])
        if j == 1:
            half = N // 2
            a, b = v[l][1, 1:half + 1, Z0:Z0 + N, :], v[l][1, half + 1:N + 1, Z0:Z0 + N, :]
            stay, move = jnp.where(ip == 1, a, b), jnp.where(ip == 1, b, a)
            xsend[l] = jnp.where(near, stay, pltpu.roll(move, CH, 2)).astype(BF16)

    def send(l, i):
        for c in copies(l, i):
            c.start()

    def fix(l, j):
        zero = jnp.zeros((N, 128), F32)
        r = zrecv[l, j].astype(F32)
        flat(l)[column(j, Z0 - 1), :] = jnp.where(iz == 1, r, zero)
        flat(l)[column(j, Z0 + N), :] = jnp.where(iz == 0, r, zero)
        r = yrecv[l, j].astype(F32)
        i, k = PART[j] if j else (0, 0)
        c = crecv[l, i, k:k + 1, :] if j else drecv[l, 0:1, :]
        for block, side in ((0, 1), (N + 1, 0)):
            v[l][j, block, Z0:Z0 + N, :] = jnp.where(ib == side, r, zero)
            corner = jnp.where(ib == side, c, zero[:1])
            v[l][j, block, Z0 - 1:Z0, :] = jnp.where(iz == 1, corner, zero[:1])
            v[l][j, block, Z0 + N:Z0 + N + 1, :] = jnp.where(iz == 0, corner, zero[:1])
        if j == 0:
            half = N // 2
            r = xrecv[l].astype(F32)
            t = pltpu.roll(r, CH, 2)
            v[l][0, 1:half + 1, Z0:Z0 + N, :] = jnp.where(ip == 0, r, t)
            v[l][0, half + 1:N + 1, Z0:Z0 + N, :] = jnp.where(ip == 0, t, r)

    def receive(l, i):
        for c in copies(l, i)[:3]:
            c.wait_recv()

    def receive_x(l):
        for c in copies(l, 0)[3:]:
            c.wait_recv()

    def load_slab(j, carry):
        x = plane0(j, j)
        for y in range(0, N, 4):
            a, b = io[y:y + 4, x].astype(F32), io[y:y + 4, x + 1].astype(F32)
            v0[j, y + 1:y + 5, Z0:Z0 + N, :] = jnp.concatenate([a, b], axis=2)
        return carry

    def weights(l, carry):
        g_copy(l).wait()
        zero = jnp.zeros((CH, CH), F32)
        for t in range(TAPS):
            e, s = t // 3, t % 3
            ga, gb, gc = (g_v[l, e, a, s].astype(F32) for a in range(3))
            rows = (jnp.concatenate([gb, gc], axis=1), jnp.concatenate([ga, gb], axis=1),
                    jnp.concatenate([zero, ga], axis=1), jnp.concatenate([gc, zero], axis=1))
            for slot in range(4):
                wt[l, CH * slot:CH * slot + CH, 128 * t:128 * t + 128] = rows[slot]
        return carry

    prev = (lax.broadcasted_iota(jnp.int32, (CHUNK, N, 128), 2) < CH).astype(jnp.int32) == ip

    def finish(l, j):
        row = bias[l:l + 1, :]
        row = jnp.concatenate([row, row], axis=1).reshape(1, 1, 128)
        x = plane0(j, j)
        for y in range(0, N, CHUNK):
            ys = slice(y, y + CHUNK)
            blocks = slice(y + 1, y + 1 + CHUNK)
            after = b_ref[j + 1, ys, :, 128:] if j < PAIRS else jnp.zeros((CHUNK, N, 128), F32)
            acc = b_ref[j, ys, :, :128] + jnp.where(prev, b_ref[j - 1, ys, :, 128:], after) + row
            half = 0.5 * acc
            act = half + half * jnp.tanh(acc * (0.7978845608028654 + 0.035677408136300125 * (acc * acc)))
            new = v[l][j, blocks, Z0:Z0 + N, :] + act
            if l + 1 < LAYERS:
                v[l + 1][j, blocks, Z0:Z0 + N, :] = new.astype(BF16).astype(F32)
            else:
                out[ys, x] = new[:, :, :CH].astype(BF16)
                out[ys, x + 1] = pltpu.roll(new, CH, 2)[:, :, :CH].astype(BF16)

    def multiply(l, j):
        parts = [v[l][j, t // 3:t // 3 + N, Z0 - 1 + t % 3:Z0 - 1 + t % 3 + N, :].reshape(N * N, 128) for t in range(TAPS)]
        prod = lax.dot_general(jnp.concatenate(parts, axis=1), wt[l], (((1,), (1,)), ((), ())), preferred_element_type=F32)
        b_ref[j] = prod.reshape(N, N, 256)

    done = 0
    for i, (j0, j1) in enumerate(LOADS):
        in_copy(i).wait()
        lax.fori_loop(j0, j1 + 1, load_slab, 0)
        while done < len(GROUPS) and GROUPS[done][1] <= j1:
            for j in range(GROUPS[done][0], GROUPS[done][1] + 1):
                stage(0, j)
            if done == 0:
                pl.semaphore_wait(barrier, len(all_peers))
            send(0, done)
            done += 1
    lax.fori_loop(0, LAYERS, weights, 0)
    bias_copy.wait()

    for n in range(LAYERS * SLABS + 2):
        for l in range(1, LAYERS):
            for i, (_, _, start, _) in enumerate(GROUPS):
                if n == (l - 1) * SLABS + start:
                    send(l, i)
        arrived = []
        for l in range(LAYERS):
            for i, (j0, j1, _, end) in enumerate(GROUPS):
                if n == max(0, (l - 1) * SLABS + end):
                    receive(l, i)
                    arrived += [(l, j) for j in range(j0, j1 + 1)]
            if n == max(0, (l - 1) * SLABS + X_END):
                receive_x(l)
                arrived.append((l, 0))
        for l in range(LAYERS):
            for j in range(1, SLABS):
                if n - l * SLABS == READY[j]:
                    finish(l, j)
                    if l + 1 < LAYERS:
                        stage(l + 1, j)
        for l, j in arrived:
            fix(l, j)
        if n < LAYERS * SLABS:
            multiply(n // SLABS, ORDER[n % SLABS])
    for l in range(LAYERS):
        for i in range(len(GROUPS)):
            for c in copies(l, i):
                c.wait_send()


def solution(mesh):
    any_spec, vmem = pl.BlockSpec(memory_space=pl.ANY), pl.BlockSpec(memory_space=pltpu.VMEM)
    copies = LAYERS * (3 * len(GROUPS) + 4)

    def local(block, kernels, biases):
        vol = jnp.transpose(block, (1, 2, 3, 0))
        g = jnp.transpose(kernels, (0, 3, 4, 5, 1, 2))
        out = pl.pallas_call(
            kernel,
            out_shape=pltpu.VMEM((N, N, N, CH), BF16),
            in_specs=[any_spec] * 3,
            out_specs=vmem,
            scratch_shapes=[pltpu.VMEM((SLABS, 26, PITCH, 128), F32)] * 3 + [
                pltpu.VMEM((SLABS, N, N, 256), F32),
                pltpu.VMEM((N, N, N, CH), BF16),
                pltpu.VMEM((LAYERS, 3, 3, 3, CH, CH), BF16),
                pltpu.VMEM((LAYERS, 256, 128 * TAPS), F32),
                pltpu.VMEM((LAYERS, SLABS, N, 128), BF16),
                pltpu.VMEM((LAYERS, SLABS, N, 128), BF16),
                pltpu.VMEM((LAYERS, SLABS, N, 128), BF16),
                pltpu.VMEM((LAYERS, SLABS, N, 128), BF16),
                pltpu.VMEM((LAYERS, N // 2, N, 128), BF16),
                pltpu.VMEM((LAYERS, N // 2, N, 128), BF16),
                pltpu.VMEM((LAYERS, len(GROUPS), 8, 128), F32),
                pltpu.VMEM((LAYERS, len(GROUPS), 8, 128), F32),
                pltpu.VMEM((LAYERS, 8, 128), F32),
                pltpu.VMEM((LAYERS, CH), F32),
                pltpu.SemaphoreType.DMA((len(LOADS),)),
                pltpu.SemaphoreType.DMA,
                pltpu.SemaphoreType.DMA((LAYERS,)),
                pltpu.SemaphoreType.DMA((copies,)),
                pltpu.SemaphoreType.DMA((copies,)),
            ],
            compiler_params=pltpu.CompilerParams(collective_id=0, has_side_effects=True, vmem_limit_bytes=52 * 2 ** 20),
        )(vol, g, biases)
        return jnp.transpose(out, (3, 0, 1, 2))

    spec = P("dp", "x", "y", "z")
    return jax.shard_map(local, mesh=mesh, in_specs=(spec, P(), P()), out_specs=spec, check_vma=False)
```

```python
import jax
import jax.numpy as jnp
from jax import lax
from jax.experimental import pallas as pl
from jax.experimental.pallas import tpu as pltpu
from jax.sharding import PartitionSpec as P

LAYERS, CH, TAPS, N = 3, 64, 9, 24
PAIRS = N // 2
SLABS = PAIRS + 1
PITCH, Z0 = 40, 8
ORDER = (1, 2, 3, 0, 4, 5, 6, 7, 8, 9, 10, 11, 12)
LOADS = ((1, 1), (2, 3), (4, 6), (7, 9), (10, 12))
FENCES = (1, 3, 5, 7, 9, 11)
CHUNK = 2
AHEAD = 0
F32, BF16 = jnp.float32, jnp.bfloat16

PLACE = {j: p for p, j in enumerate(ORDER)}
READY = {j: max(PLACE[k] for k in (j - 1, j, j + 1) if k in PLACE) + 1 for j in range(1, SLABS)}
POINTS = [SLABS * l + p for l in range(-1, 2) for p in FENCES]


def _groups():
    found = {}
    for j in range(1, SLABS):
        key = (min(p for p in POINTS if p > READY[j]), max(p for p in POINTS if p <= SLABS + PLACE[j] - AHEAD))
        found.setdefault(key, []).append(j)
    return [(min(js), max(js), start, end) for (start, end), js in sorted(found.items(), key=lambda kv: kv[1])]


GROUPS = _groups()
X_END = max(p for p in POINTS if p <= SLABS + PLACE[0] - AHEAD)
PART = {j: (i, j - g[0]) for i, g in enumerate(GROUPS) for j in range(g[0], g[1] + 1)}


def kernel(vol, g_hbm, bias_hbm, out, v0, v1, v2, b_ref, io, g_v, wt, zsend, zrecv, ysend, yrecv, xsend, xrecv,
           csend, crecv, drecv, bias, in_sem, bias_sem, g_sem, send_sem, recv_sem):
    v = (v0, v1, v2)
    ip, ib, iz = lax.axis_index("y"), lax.axis_index("x"), lax.axis_index("z")

    def peer(*axes):
        mine = {"y": ip, "x": ib, "z": iz}
        return {a: 1 - mine[a] for a in axes}

    barrier = pltpu.get_barrier_semaphore()
    all_peers = (("x",), ("y",), ("z",), ("x", "y"), ("x", "z"), ("y", "z"), ("x", "y", "z"))
    for axes in all_peers:
        pl.semaphore_signal(barrier, inc=1, device_id=peer(*axes), device_id_type=pl.DeviceIdType.MESH)

    def plane0(j0, j1):
        return 2 * (ip * (j0 - 1) + (1 - ip) * (PAIRS - j1))

    def in_copy(i):
        j0, j1 = LOADS[i]
        planes = pl.ds(plane0(j0, j1), 2 * (j1 - j0 + 1))
        return pltpu.make_async_copy(vol.at[:, planes], io.at[:, planes], in_sem.at[i])

    def g_copy(l):
        return pltpu.make_async_copy(g_hbm.at[l], g_v.at[l], g_sem.at[l])

    for i in range(len(LOADS)):
        in_copy(i).start()
    for l in range(LAYERS):
        g_copy(l).start()
    bias_copy = pltpu.make_async_copy(bias_hbm, bias, bias_sem)
    bias_copy.start()

    kinds = 3 * len(GROUPS) + 4

    def remote(l, slot, src, dst, *axes):
        return pltpu.make_async_remote_copy(
            src_ref=src, dst_ref=dst, send_sem=send_sem.at[l * kinds + slot], recv_sem=recv_sem.at[l * kinds + slot],
            device_id=peer(*axes), device_id_type=pl.DeviceIdType.MESH)

    def copies(l, i):
        j0, j1 = GROUPS[i][:2]
        slabs = pl.ds(j0, j1 - j0 + 1)
        got = [
            remote(l, 3 * i, ysend.at[l, slabs], yrecv.at[l, slabs], "x"),
            remote(l, 3 * i + 1, zsend.at[l, slabs], zrecv.at[l, slabs], "z"),
            remote(l, 3 * i + 2, csend.at[l, i], crecv.at[l, i], "x", "z"),
        ]
        if i == 0:
            n = 3 * len(GROUPS)
            got += [
                remote(l, n, xsend.at[l], xrecv.at[l], "y"),
                remote(l, n + 1, ysend.at[l, 1], yrecv.at[l, 0], "x", "y"),
                remote(l, n + 2, zsend.at[l, 1], zrecv.at[l, 0], "y", "z"),
                remote(l, n + 3, csend.at[l, 0], drecv.at[l], "x", "y", "z"),
            ]
        return got

    near = (lax.broadcasted_iota(jnp.int32, (N // 2, N, 128), 2) < CH).astype(jnp.int32) == ip

    def flat(l):
        return v[l].reshape(SLABS * (N + 2) * PITCH, 128)

    def column(j, row):
        return pl.ds((j * (N + 2) + 1) * PITCH + row, N, stride=PITCH)

    def stage(l, j):
        lo, hi = flat(l)[column(j, Z0), :], flat(l)[column(j, Z0 + N - 1), :]
        edge = jnp.where(iz == 0, hi, lo)
        zsend[l, j] = edge.astype(BF16)
        ysend[l, j] = jnp.where(ib == 0, v[l][j, N, Z0:Z0 + N, :], v[l][j, 1, Z0:Z0 + N, :]).astype(BF16)
        i, r = PART[j]
        csend[l, i, r:r + 1] = jnp.where(ib == 0, edge[N - 1:N], edge[0:1])
        if j == 1:
            half = N // 2
            a, b = v[l][1, 1:half + 1, Z0:Z0 + N, :], v[l][1, half + 1:N + 1, Z0:Z0 + N, :]
            stay, move = jnp.where(ip == 1, a, b), jnp.where(ip == 1, b, a)
            xsend[l] = jnp.where(near, stay, pltpu.roll(move, CH, 2)).astype(BF16)

    def send(l, i):
        for c in copies(l, i):
            c.start()

    def fix(l, j):
        zero = jnp.zeros((N, 128), F32)
        r = zrecv[l, j].astype(F32)
        flat(l)[column(j, Z0 - 1), :] = jnp.where(iz == 1, r, zero)
        flat(l)[column(j, Z0 + N), :] = jnp.where(iz == 0, r, zero)
        r = yrecv[l, j].astype(F32)
        i, k = PART[j] if j else (0, 0)
        c = crecv[l, i, k:k + 1, :] if j else drecv[l, 0:1, :]
        for block, side in ((0, 1), (N + 1, 0)):
            v[l][j, block, Z0:Z0 + N, :] = jnp.where(ib == side, r, zero)
            corner = jnp.where(ib == side, c, zero[:1])
            v[l][j, block, Z0 - 1:Z0, :] = jnp.where(iz == 1, corner, zero[:1])
            v[l][j, block, Z0 + N:Z0 + N + 1, :] = jnp.where(iz == 0, corner, zero[:1])
        if j == 0:
            half = N // 2
            r = xrecv[l].astype(F32)
            t = pltpu.roll(r, CH, 2)
            v[l][0, 1:half + 1, Z0:Z0 + N, :] = jnp.where(ip == 0, r, t)
            v[l][0, half + 1:N + 1, Z0:Z0 + N, :] = jnp.where(ip == 0, t, r)

    def receive(l, i):
        for c in copies(l, i)[:3]:
            c.wait_recv()

    def receive_x(l):
        for c in copies(l, 0)[3:]:
            c.wait_recv()

    def load_slab(j, carry):
        x = plane0(j, j)
        for y in range(0, N, 4):
            a, b = io[y:y + 4, x].astype(F32), io[y:y + 4, x + 1].astype(F32)
            v0[j, y + 1:y + 5, Z0:Z0 + N, :] = jnp.concatenate([a, b], axis=2)
        return carry

    def weights(l, carry):
        g_copy(l).wait()
        zero = jnp.zeros((CH, CH), F32)
        for t in range(TAPS):
            e, s = t // 3, t % 3
            ga, gb, gc = (g_v[l, e, a, s].astype(F32) for a in range(3))
            rows = (jnp.concatenate([gb, gc], axis=1), jnp.concatenate([ga, gb], axis=1),
                    jnp.concatenate([zero, ga], axis=1), jnp.concatenate([gc, zero], axis=1))
            for slot in range(4):
                wt[l, CH * slot:CH * slot + CH, 128 * t:128 * t + 128] = rows[slot]
        return carry

    prev = (lax.broadcasted_iota(jnp.int32, (CHUNK, N, 128), 2) < CH).astype(jnp.int32) == ip

    def finish(l, j):
        row = bias[l:l + 1, :]
        row = jnp.concatenate([row, row], axis=1).reshape(1, 1, 128)
        x = plane0(j, j)
        for y in range(0, N, CHUNK):
            ys = slice(y, y + CHUNK)
            blocks = slice(y + 1, y + 1 + CHUNK)
            after = b_ref[j + 1, ys, :, 128:] if j < PAIRS else jnp.zeros((CHUNK, N, 128), F32)
            acc = b_ref[j, ys, :, :128] + jnp.where(prev, b_ref[j - 1, ys, :, 128:], after) + row
            half = 0.5 * acc
            act = half + half * jnp.tanh(acc * (0.7978845608028654 + 0.035677408136300125 * (acc * acc)))
            new = v[l][j, blocks, Z0:Z0 + N, :] + act
            if l + 1 < LAYERS:
                v[l + 1][j, blocks, Z0:Z0 + N, :] = new.astype(BF16).astype(F32)
            else:
                out[ys, x] = new[:, :, :CH].astype(BF16)
                out[ys, x + 1] = pltpu.roll(new, CH, 2)[:, :, :CH].astype(BF16)

    def multiply(l, j):
        parts = [v[l][j, t // 3:t // 3 + N, Z0 - 1 + t % 3:Z0 - 1 + t % 3 + N, :].reshape(N * N, 128) for t in range(TAPS)]
        prod = lax.dot_general(jnp.concatenate(parts, axis=1), wt[l], (((1,), (1,)), ((), ())), preferred_element_type=F32)
        b_ref[j] = prod.reshape(N, N, 256)

    done = 0
    for i, (j0, j1) in enumerate(LOADS):
        in_copy(i).wait()
        lax.fori_loop(j0, j1 + 1, load_slab, 0)
        while done < len(GROUPS) and GROUPS[done][1] <= j1:
            for j in range(GROUPS[done][0], GROUPS[done][1] + 1):
                stage(0, j)
            if done == 0:
                pl.semaphore_wait(barrier, len(all_peers))
            send(0, done)
            done += 1
    lax.fori_loop(0, LAYERS, weights, 0)
    bias_copy.wait()

    for n in range(LAYERS * SLABS + 2):
        for l in range(1, LAYERS):
            for i, (_, _, start, _) in enumerate(GROUPS):
                if n == (l - 1) * SLABS + start:
                    send(l, i)
        arrived = []
        for l in range(LAYERS):
            for i, (j0, j1, _, end) in enumerate(GROUPS):
                if n == max(0, (l - 1) * SLABS + end):
                    receive(l, i)
                    arrived += [(l, j) for j in range(j0, j1 + 1)]
            if n == max(0, (l - 1) * SLABS + X_END):
                receive_x(l)
                arrived.append((l, 0))
        if n == (LAYERS - 2) * SLABS + max(end for _, _, _, end in GROUPS):
            for l in range(LAYERS):
                for i in range(len(GROUPS)):
                    for c in copies(l, i):
                        c.wait_send()
        for l in range(LAYERS):
            for j in range(1, SLABS):
                if n - l * SLABS == READY[j]:
                    finish(l, j)
                    if l + 1 < LAYERS:
                        stage(l + 1, j)
        for l, j in arrived:
            fix(l, j)
        if n < LAYERS * SLABS:
            multiply(n // SLABS, ORDER[n % SLABS])


def solution(mesh):
    any_spec, vmem = pl.BlockSpec(memory_space=pl.ANY), pl.BlockSpec(memory_space=pltpu.VMEM)
    copies = LAYERS * (3 * len(GROUPS) + 4)

    def local(block, kernels, biases):
        vol = jnp.transpose(block, (1, 2, 3, 0))
        g = jnp.transpose(kernels, (0, 3, 4, 5, 1, 2))
        out = pl.pallas_call(
            kernel,
            out_shape=pltpu.VMEM((N, N, N, CH), BF16),
            in_specs=[any_spec] * 3,
            out_specs=vmem,
            scratch_shapes=[pltpu.VMEM((SLABS, 26, PITCH, 128), F32)] * 3 + [
                pltpu.VMEM((SLABS, N, N, 256), F32),
                pltpu.VMEM((N, N, N, CH), BF16),
                pltpu.VMEM((LAYERS, 3, 3, 3, CH, CH), BF16),
                pltpu.VMEM((LAYERS, 256, 128 * TAPS), F32),
                pltpu.VMEM((LAYERS, SLABS, N, 128), BF16),
                pltpu.VMEM((LAYERS, SLABS, N, 128), BF16),
                pltpu.VMEM((LAYERS, SLABS, N, 128), BF16),
                pltpu.VMEM((LAYERS, SLABS, N, 128), BF16),
                pltpu.VMEM((LAYERS, N // 2, N, 128), BF16),
                pltpu.VMEM((LAYERS, N // 2, N, 128), BF16),
                pltpu.VMEM((LAYERS, len(GROUPS), 8, 128), F32),
                pltpu.VMEM((LAYERS, len(GROUPS), 8, 128), F32),
                pltpu.VMEM((LAYERS, 8, 128), F32),
                pltpu.VMEM((LAYERS, CH), F32),
                pltpu.SemaphoreType.DMA((len(LOADS),)),
                pltpu.SemaphoreType.DMA,
                pltpu.SemaphoreType.DMA((LAYERS,)),
                pltpu.SemaphoreType.DMA((copies,)),
                pltpu.SemaphoreType.DMA((copies,)),
            ],
            compiler_params=pltpu.CompilerParams(collective_id=0, has_side_effects=True, vmem_limit_bytes=52 * 2 ** 20),
        )(vol, g, biases)
        return jnp.transpose(out, (3, 0, 1, 2))

    spec = P("dp", "x", "y", "z")
    return jax.shard_map(local, mesh=mesh, in_specs=(spec, P(), P()), out_specs=spec, check_vma=False)
```
